32 devices in a mesh: rows: 8 (over z, x), grp: 4 (over y, core).
Axes of the slice: x: 2, y: 2, z: 4, core: 2. Of those that a mesh axis runs over, the one named last changes fastest.
Arguments:
- queries: bfloat16 [2048, 1024], P('rows'), may hold values from -12 to 12
- passages: bfloat16 [8192, 1024], P(('rows', 'grp')), may hold values from -12 to 12
- positive: int32 [2048], P('rows'), may hold values from 0 to 8191
Outputs:
- losses: float32 [2048], P('rows')
- grad_queries: float32 [2048, 1024], P('rows')
- grad_passages: float32 [8192, 1024], P(('rows', 'grp'))
The draws below stay inside these ranges and needn't reach their ends.
All inputs are finite; a program needn't handle non-finite values.
Results may differ from the reference program's by a relative error of at most 0.0015.
Values may be sent and summed in bfloat16 or wider, within the bound.
A program may use at most 128 MiB of HBM per device.

```python
import math
import jax
import jax.numpy as jnp
from jax import lax

D = 1024
NQ = 2048
NP = 8192


def topic_axes(key):
    topic_key = jax.random.fold_in(jax.random.fold_in(key, 91), 1)
    axes_all = jax.random.normal(topic_key, (64, D), jnp.float32)
    return axes_all / jnp.sqrt(jnp.sum(axes_all * axes_all, axis=1, keepdims=True))


def draw_queries(key, part):
    key_base = jax.random.fold_in(key, 11)
    key_scale = jax.random.fold_in(key, 12)
    key_topic = jax.random.fold_in(key, 13)
    key_amount = jax.random.fold_in(key, 14)
    axes_all = topic_axes(key)
    topic_ids = jax.random.randint(key_topic, (NQ,), 0, 64)
    amounts = jax.random.uniform(key_amount, (NQ, 1), jnp.float32, 1.0, 2.0)
    topical = amounts * jnp.take(axes_all, topic_ids, axis=0)
    values = jax.random.normal(key_base, (NQ, D), jnp.float32)
    scales = jnp.exp(jax.random.uniform(key_scale, (NQ, 1), jnp.float32, 0.0, math.log(10.0)))
    values = 0.03 * scales * values + topical
    return jnp.clip(values, -12.0, 12.0).astype(jnp.bfloat16)


def draw_passages(key, part):
    key_base = jax.random.fold_in(key, 21)
    key_scale = jax.random.fold_in(key, 22)
    key_topic = jax.random.fold_in(key, 25)
    axes_all = topic_axes(key)
    topic_ids = jax.random.randint(key_topic, (NP,), 0, 64)
    topical = 2.0 * jnp.take(axes_all, topic_ids, axis=0)
    values = jax.random.normal(key_base, (NP, D), jnp.float32)
    scales = jnp.exp(jax.random.uniform(key_scale, (NP, 1), jnp.float32, 0.0, math.log(10.0)))
    values = 0.03 * scales * values + topical
    return jnp.clip(values, -12.0, 12.0).astype(jnp.bfloat16)


def touch_ends(drawn, rng, least, high):
    place = [jax.random.randint(jax.random.fold_in(rng, axis), (), 0, length) for axis, length in enumerate(drawn.shape)]
    longest = drawn.shape.index(max(drawn.shape))
    beside = place[:longest] + [(place[longest] + 1) % drawn.shape[longest]] + place[longest + 1:]
    return drawn.at[tuple(place)].set(least).at[tuple(beside)].set(high)


def setup_inputs(seed: int = 0) -> dict:
    seeds = jax.random.split(jax.random.key(seed), 4)
    return {
        "queries": draw_queries(jax.random.fold_in(seeds[3], 71), 0),
        "passages": draw_passages(jax.random.fold_in(seeds[3], 71), 0),
        "positive": touch_ends(jax.random.randint(seeds[2], (NQ,), 0, NP), jax.random.fold_in(seeds[2], 1), 0, NP - 1).astype(jnp.int32),
    }


def reference(queries, passages, positive):
    total_q = queries.shape[0]
    width = queries.shape[1]
    total_p = passages.shape[0]
    block_rows = math.gcd(total_q, 512)
    query_blocks = queries.reshape(total_q // block_rows, block_rows, width)
    pos_blocks = positive.reshape(total_q // block_rows, block_rows)

    def one_block(accum, inputs):
        query_block, pos_block = inputs
        scores = jnp.dot(query_block, passages.T, preferred_element_type=jnp.float32)
        row_max = jnp.max(scores, axis=1)
        log_total = row_max + jnp.log(jnp.sum(jnp.exp(scores - row_max[:, None]), axis=1))
        chosen = jnp.take_along_axis(scores, pos_block[:, None].astype(jnp.int32), axis=1)[:, 0]
        block_loss = log_total - chosen
        weights = jnp.exp(scores - log_total[:, None]).astype(jnp.bfloat16)
        grad_block = jnp.dot(weights, passages, preferred_element_type=jnp.float32)
        grad_block = grad_block - jnp.take(passages, pos_block, axis=0).astype(jnp.float32)
        accum = accum + jnp.dot(weights.T, query_block, preferred_element_type=jnp.float32)
        return accum, (block_loss, grad_block)

    start_grad = jnp.zeros((total_p, width), jnp.float32)
    grad_passages, (losses, grad_queries) = lax.scan(one_block, start_grad, (query_blocks, pos_blocks))
    grad_passages = grad_passages - jnp.zeros((total_p, width), jnp.float32).at[positive].add(queries.astype(jnp.float32))
    return losses.reshape(total_q), grad_queries.reshape(total_q, width), grad_passages
```

```python
import functools

import jax
import jax.numpy as jnp
from jax import lax
from jax.experimental import pallas as pl
from jax.experimental.pallas import tpu as pltpu
from jax.sharding import PartitionSpec as P

lowest = -1e30
MESH = pl.DeviceIdType.MESH
F32 = jnp.float32
BF16 = jnp.bfloat16


def dot_nt(a, b):
    return lax.dot_general(a, b, (((1,), (1,)), ((), ())), preferred_element_type=F32)


def dot_nn(a, b):
    return jnp.dot(a, b, preferred_element_type=F32)


def kernel(
    R, G, q_hbm, p_hbm, pos_col_ref, pos_row_ref,
    loss_ref, gq_ref, gp_ref,
    p_all, q_all, pos_all, lse_all, stats, stats_in, lse_buf,
    acc, hit_acc, m_ref, l_ref, c_ref, s_keep, w_keep,
    got_core, half_sum, got_y, done_half, got_half,
    local_sem, p_send, p_recv, q_send, q_recv, f_send, f_recv,
    pos_send, pos_recv, lse_send, lse_recv, st_send, st_recv,
    x_send, x_recv, y_send, y_recv,
):
    r = lax.axis_index("rows")
    g = lax.axis_index("grp")
    half_ring = R // 2
    _, Pd, D = p_all.shape
    Rq = q_all.shape[1]
    tile = min(256, D)
    z, x = r // 2, r % 2
    place = z + x * (R - 1 - 2 * z)

    def row_of(where):
        far = where // half_ring
        return 2 * (where + far * (R - 1 - 2 * where)) + far

    def origin(way, d):
        return row_of((place + (2 * way - 1) * d + R) % R)

    right, left = row_of((place + 1) % R), row_of((place + R - 1) % R)
    target = (right, left)
    core = g % 2
    partner = g + 1 - 2 * core

    def to_row(row):
        return (row, g)

    def to_grp(col):
        return (r, col)

    def remote(src, dst, send, recv, device):
        return pltpu.make_async_remote_copy(
            src_ref=src, dst_ref=dst, send_sem=send, recv_sem=recv,
            device_id=device, device_id_type=MESH,
        )

    load_p = pltpu.make_async_copy(p_hbm, p_all.at[r], local_sem.at[0])
    load_q = pltpu.make_async_copy(q_hbm, q_all.at[r], local_sem.at[1])
    load_p.start()
    load_q.start()

    barrier = pltpu.get_barrier_semaphore()
    for k in range(1, R):
        pl.semaphore_signal(barrier, inc=1, device_id=to_row((r + k) % R), device_id_type=MESH)
    for k in range(1, G):
        pl.semaphore_signal(barrier, inc=1, device_id=to_grp((g + k) % G), device_id_type=MESH)
    pl.semaphore_wait(barrier, R - 1 + G - 1)

    pc = Pd // 2

    def p_copy(way, src, d, chunk):
        piece = p_all.at[src, pl.ds(chunk * pc, pc)]
        return remote(piece, piece, p_send.at[way, d, chunk], p_recv.at[way, d, chunk],
                      to_row(target[way]))

    qc = Rq // 4

    def q_copy(way, src, d, chunk):
        piece = q_all.at[src, pl.ds(pl.multiple_of(core * (2 * qc) + chunk * qc, qc), qc)]
        return remote(piece, piece, q_send.at[way, d, chunk], q_recv.at[way, d, chunk],
                      to_row(target[way]))

    def f_copy(way, src, d, chunk, whose):
        piece = q_all.at[src, pl.ds(pl.multiple_of(whose * (2 * qc) + chunk * qc, qc), qc)]
        return remote(piece, piece, f_send.at[way, d, chunk], f_recv.at[way, d, chunk],
                      to_grp(partner))

    load_p.wait()
    for chunk in range(2):
        for way in range(2):
            p_copy(way, r, 1, chunk).start()
    load_q.wait()

    def pos_copy(k, src):
        return remote(pos_row_ref, pos_all.at[src], pos_send.at[k], pos_recv.at[k],
                      to_row((r + k) % R))

    for k in range(1, R):
        pos_copy(k, r).start()
    pos_all[r] = pos_row_ref[...]

    m_ref[...] = jnp.full((Rq, 1), lowest, F32)
    l_ref[...] = jnp.zeros((Rq, 1), F32)
    c_ref[...] = jnp.zeros((Rq, 1), F32)
    acc[...] = jnp.zeros((Rq, D), F32)
    hit_acc[...] = jnp.zeros((Rq, D), F32)

    def use_passages(u):
        block = p_all.at[u]
        s = dot_nt(q_all[r], block[...])
        column = (u * G + g) * Pd + lax.broadcasted_iota(jnp.int32, (Rq, Pd), 1)
        hit = pos_col_ref[...] == column
        c_ref[...] += jnp.sum(jnp.where(hit, s, 0.0), axis=1, keepdims=True)
        old = m_ref[...]
        new = jnp.maximum(old, jnp.max(s, axis=1, keepdims=True))
        scale = jnp.exp(old - new)
        w = jnp.exp(s - new)
        l_ref[...] = l_ref[...] * scale + jnp.sum(w, axis=1, keepdims=True)
        m_ref[...] = new
        w = w.astype(BF16)
        one = jnp.where(hit, 1.0, 0.0).astype(BF16)
        for t in range(0, D, tile):
            cols = pl.ds(t, tile)
            acc[:, cols] = acc[:, cols] * scale + dot_nn(w, block[:, cols])
            hit_acc[:, cols] += dot_nn(one, block[:, cols])

    use_passages(r)

    def p_step(d, carry):
        for chunk in range(2):
            for way in range(2):
                src = origin(way, d)
                p_copy(way, src, d, chunk).wait_recv()
                if chunk == way:
                    p_copy(way, src, d + 1, chunk).start()
                else:
                    @pl.when(d + 1 < half_ring)
                    def _():
                        p_copy(way, src, d + 1, chunk).start()

        @pl.when(d + 1 == half_ring)
        def _():
            for chunk in range(2):
                for way in range(2):
                    q_copy(way, r, 1, chunk).start()

        for way in range(2):
            use_passages(origin(way, d))
        return carry

    lax.fori_loop(1, half_ring, p_step, 0)
    last = origin(0, half_ring)
    for way in range(2):
        p_copy(way, last, half_ring, way).wait_recv()
    use_passages(last)

    lane = lax.broadcasted_iota(jnp.int32, (Rq, 128), 1)
    cols = jnp.where(lane == 0, m_ref[...], jnp.where(lane == 1, l_ref[...], c_ref[...]))
    stats[...] = cols.T[0:8, :]

    def st_copy(k, src):
        return remote(stats, stats_in.at[src], st_send.at[k], st_recv.at[k],
                      to_grp((g + k) % G))

    for k in range(1, G):
        st_copy(k, g).start()
    for k in range(1, G):
        st_copy(k, (g - k + G) % G).wait_recv()
    stats_in[g] = stats[...]
    parts = [stats_in[k] for k in range(G)]
    top = functools.reduce(jnp.maximum, [v[0:1] for v in parts])
    total = functools.reduce(jnp.add, [v[1:2] * jnp.exp(v[0:1] - top) for v in parts])
    lse = top + jnp.log(total)
    loss_ref[...] = lse - functools.reduce(jnp.add, [v[2:3] for v in parts])
    lse_buf[...] = jnp.broadcast_to(lse, (8, Rq))

    def lse_copy(k, src):
        return remote(lse_buf, lse_all.at[src], lse_send.at[k], lse_recv.at[k],
                      to_row((r + k) % R))

    for k in range(1, R):
        lse_copy(k, r).start()
    lse_all[r] = lse_buf[...]

    lse_col = jnp.broadcast_to(lse, (128, Rq)).T[:, 0:1]
    hr = Rq // 2
    final = jnp.exp(m_ref[...] - lse_col)
    acc[...] = acc[...] * final - hit_acc[...]
    mine = pl.ds(pl.multiple_of(core * hr, hr), hr)
    other = pl.ds(pl.multiple_of((1 - core) * hr, hr), hr)
    core_copy = remote(acc.at[other], got_core, x_send.at[0], x_recv.at[0], to_grp(partner))
    core_copy.start()
    core_copy.wait_recv()
    half_sum[...] = acc[mine] + got_core[...]

    def y_copy(k):
        return remote(half_sum, got_y.at[k - 1], y_send.at[k], y_recv.at[k],
                      to_grp((g + 2 * k) % G))

    for k in range(1, G // 2):
        y_copy(k).start()

    gp_ref[...] = jnp.zeros((Pd, D), F32)
    base = (r * G + g) * Pd

    def use_queries(u):
        block = q_all.at[u]
        s_keep[u] = dot_nt(p_all[r], block[...])
        row = base + lax.broadcasted_iota(jnp.int32, (Pd, Rq), 0)
        one = jnp.where(row == pos_all[u][0:1], 1.0, 0.0).astype(BF16)
        for t in range(0, D, tile):
            c = pl.ds(t, tile)
            gp_ref[:, c] -= dot_nn(one, block[:, c])

    for k in range(1, R):
        pos_copy(k, (r - k + R) % R).wait_recv()
    use_queries(r)

    def q_step(d, carry):
        for chunk in range(2):
            for way in range(2):
                src = origin(way, d)
                q_copy(way, src, d, chunk).wait_recv()
                if chunk == way:
                    q_copy(way, src, d + 1, chunk).start()
                else:
                    @pl.when(d + 1 < half_ring)
                    def _():
                        q_copy(way, src, d + 1, chunk).start()
                f_copy(way, src, d, chunk, core).start()
        for way in range(2):
            src = origin(way, d)
            for chunk in range(2):
                f_copy(way, src, d, chunk, 1 - core).wait_recv()
            use_queries(src)
        return carry

    lax.fori_loop(1, half_ring, q_step, 0)
    for way in range(2):
        q_copy(way, last, half_ring, way).wait_recv()
        f_copy(way, last, half_ring, way, core).start()

    for k in range(1, G // 2):
        y_copy(k).wait_recv()
    whole = half_sum[...]
    for k in range(1, G // 2):
        whole = whole + got_y[k - 1]
    done_half[...] = whole
    back_copy = remote(done_half, got_half, x_send.at[1], x_recv.at[1], to_grp(partner))
    back_copy.start()
    gq_ref[mine] = whole

    for way in range(2):
        f_copy(way, last, half_ring, way, 1 - core).wait_recv()
    use_queries(last)
    for k in range(1, R):
        lse_copy(k, (r - k + R) % R).wait_recv()

    def weigh(u, carry):
        at = pl.ds(pl.multiple_of(u * Rq, Rq), Rq)
        w_keep[:, at] = jnp.exp(s_keep[u] - lse_all[u][0:1]).astype(BF16)
        return carry

    lax.fori_loop(0, R, weigh, 0)

    def passages_tile(t, carry):
        c = pl.ds(pl.multiple_of(t * tile, tile), tile)
        q_cols = q_all[:, :, c].reshape(R * Rq, tile)
        gp_ref[:, c] += dot_nn(w_keep[...], q_cols)
        return carry

    lax.fori_loop(0, D // tile, passages_tile, 0)

    back_copy.wait_recv()
    gq_ref[other] = got_half[...]

    def drain(d, carry):
        for chunk in range(2):
            for way in range(2):
                src = origin(way, d)

                def settle():
                    p_copy(way, src, d, chunk).wait_send()
                    q_copy(way, src, d, chunk).wait_send()
                    f_copy(way, src, d, chunk, core).wait_send()

                if chunk == way:
                    settle()
                else:
                    pl.when(d < half_ring)(settle)
        return carry

    lax.fori_loop(1, half_ring + 1, drain, 0)
    for k in range(1, R):
        pos_copy(k, r).wait_send()
        lse_copy(k, r).wait_send()
    for k in range(1, G):
        st_copy(k, g).wait_send()
    for k in range(1, G // 2):
        y_copy(k).wait_send()
    core_copy.wait_send()
    back_copy.wait_send()


def local(R, G, queries, passages, positive):
    Rq, D = queries.shape
    Pd = passages.shape[0]
    pos_col = positive[:, None]
    pos_row = jnp.broadcast_to(positive[None, :], (8, Rq))
    ring = (2, R // 2 + 1, 2)
    sem = pltpu.SemaphoreType.DMA
    vmem = pltpu.VMEM
    losses, gq, gp = pl.pallas_call(
        functools.partial(kernel, R, G),
        out_shape=(
            jax.ShapeDtypeStruct((1, Rq), F32),
            jax.ShapeDtypeStruct((Rq, D), F32),
            jax.ShapeDtypeStruct((Pd, D), F32),
        ),
        in_specs=[
            pl.BlockSpec(memory_space=pl.ANY),
            pl.BlockSpec(memory_space=pl.ANY),
            pl.BlockSpec(memory_space=vmem),
            pl.BlockSpec(memory_space=vmem),
        ],
        out_specs=[pl.BlockSpec(memory_space=vmem)] * 3,
        scratch_shapes=[
            vmem((R, Pd, D), BF16),
            vmem((R, Rq, D), BF16),
            vmem((R, 8, Rq), jnp.int32),
            vmem((R, 8, Rq), F32),
            vmem((8, Rq), F32),
            vmem((G, 8, Rq), F32),
            vmem((8, Rq), F32),
            vmem((Rq, D), F32),
            vmem((Rq, D), F32),
            vmem((Rq, 1), F32),
            vmem((Rq, 1), F32),
            vmem((Rq, 1), F32),
            vmem((R, Pd, Rq), F32),
            vmem((Pd, R * Rq), BF16),
            vmem((Rq // 2, D), F32),
            vmem((Rq // 2, D), F32),
            vmem((G // 2 - 1, Rq // 2, D), F32),
            vmem((Rq // 2, D), F32),
            vmem((Rq // 2, D), F32),
            sem((2,)),
            sem(ring), sem(ring), sem(ring), sem(ring), sem(ring), sem(ring),
            sem((R,)), sem((R,)), sem((R,)), sem((R,)), sem((G,)), sem((G,)),
            sem((2,)), sem((2,)), sem((G // 2,)), sem((G // 2,)),
        ],
        compiler_params=pltpu.CompilerParams(
            collective_id=0, has_side_effects=True, vmem_limit_bytes=60 * 1024 * 1024
        ),
        name="infonce",
    )(queries, passages, pos_col, pos_row)
    return losses[0], gq, gp


def solution(mesh):
    R, G = mesh.shape["rows"], mesh.shape["grp"]
    return jax.shard_map(
        functools.partial(local, R, G),
        mesh=mesh,
        in_specs=(P("rows", None), P(("rows", "grp"), None), P("rows")),
        out_specs=(P("rows"), P("rows", None), P(("rows", "grp"), None)),
        check_vma=False,
    )
```

```python
import functools

import jax
import jax.numpy as jnp
from jax import lax
from jax.experimental import pallas as pl
from jax.experimental.pallas import tpu as pltpu
from jax.sharding import PartitionSpec as P

lowest = -1e30
MESH = pl.DeviceIdType.MESH
F32 = jnp.float32
BF16 = jnp.bfloat16


def dot_nt(a, b):
    return lax.dot_general(a, b, (((1,), (1,)), ((), ())), preferred_element_type=F32)


def dot_nn(a, b):
    return jnp.dot(a, b, preferred_element_type=F32)


def kernel(
    R, G, q_hbm, p_hbm, pos_ref,
    loss_ref, gq_ref, gp_ref,
    p_all, q_all, pos_all, lse_all, stats, stats_in, lse_buf,
    acc, hit_acc, m_ref, l_ref, c_ref, pos_col_ref, pos_row_ref,
    got_core, half_sum, got_y, done_half, got_half,
    local_sem, p_send, p_recv, q_send, q_recv, f_send, f_recv,
    pos_send, pos_recv, lse_send, lse_recv, st_send, st_recv,
    x_send, x_recv, y_send, y_recv,
):
    r = lax.axis_index("rows")
    g = lax.axis_index("grp")
    half_ring = R // 2
    _, Pd, D = p_all.shape
    Rq = q_all.shape[1]
    tile = min(256, D)
    z, x = r // 2, r % 2
    place = z + x * (R - 1 - 2 * z)

    def row_of(where):
        far = where // half_ring
        return 2 * (where + far * (R - 1 - 2 * where)) + far

    def origin(way, d):
        return row_of((place + (2 * way - 1) * d + R) % R)

    right, left = row_of((place + 1) % R), row_of((place + R - 1) % R)
    target = (right, left)
    core = g % 2
    partner = g + 1 - 2 * core

    def to_row(row):
        return (row, g)

    def to_grp(col):
        return (r, col)

    def remote(src, dst, send, recv, device):
        return pltpu.make_async_remote_copy(
            src_ref=src, dst_ref=dst, send_sem=send, recv_sem=recv,
            device_id=device, device_id_type=MESH,
        )

    load_p = pltpu.make_async_copy(p_hbm, p_all.at[r], local_sem.at[0])
    load_q = pltpu.make_async_copy(q_hbm, q_all.at[r], local_sem.at[1])
    load_p.start()
    load_q.start()

    barrier = pltpu.get_barrier_semaphore()
    for k in range(1, R):
        pl.semaphore_signal(barrier, inc=1, device_id=to_row((r + k) % R), device_id_type=MESH)
    for k in range(1, G):
        pl.semaphore_signal(barrier, inc=1, device_id=to_grp((g + k) % G), device_id_type=MESH)
    pl.semaphore_wait(barrier, R - 1 + G - 1)

    pc = Pd // 2

    def p_copy(way, src, d, chunk):
        piece = p_all.at[src, pl.ds(chunk * pc, pc)]
        return remote(piece, piece, p_send.at[way, d, chunk], p_recv.at[way, d, chunk],
                      to_row(target[way]))

    qc = Rq // 4

    def q_copy(way, src, d, chunk):
        piece = q_all.at[src, pl.ds(pl.multiple_of(core * (2 * qc) + chunk * qc, qc), qc)]
        return remote(piece, piece, q_send.at[way, d, chunk], q_recv.at[way, d, chunk],
                      to_row(target[way]))

    def f_copy(way, src, d, chunk, whose):
        piece = q_all.at[src, pl.ds(pl.multiple_of(whose * (2 * qc) + chunk * qc, qc), qc)]
        return remote(piece, piece, f_send.at[way, d, chunk], f_recv.at[way, d, chunk],
                      to_grp(partner))

    load_p.wait()
    for chunk in range(2):
        for way in range(2):
            p_copy(way, r, 1, chunk).start()
    load_q.wait()

    def pos_copy(k, src):
        return remote(pos_row_ref, pos_all.at[src], pos_send.at[k], pos_recv.at[k],
                      to_row((r + k) % R))

    pos_row_ref[...] = jnp.broadcast_to(pos_ref[...], (8, Rq))
    pos_col_ref[...] = jnp.broadcast_to(pos_ref[...], (128, Rq)).T[:, 0:1]
    for k in range(1, R):
        pos_copy(k, r).start()
    pos_all[r] = pos_row_ref[...]

    m_ref[...] = jnp.full((Rq, 1), lowest, F32)
    l_ref[...] = jnp.zeros((Rq, 1), F32)
    c_ref[...] = jnp.zeros((Rq, 1), F32)
    acc[...] = jnp.zeros((Rq, D), F32)
    hit_acc[...] = jnp.zeros((Rq, D), F32)

    def use_passages(u):
        block = p_all.at[u]
        s = dot_nt(q_all[r], block[...])
        column = (u * G + g) * Pd + lax.broadcasted_iota(jnp.int32, (Rq, Pd), 1)
        hit = pos_col_ref[...] == column
        c_ref[...] += jnp.sum(jnp.where(hit, s, 0.0), axis=1, keepdims=True)
        old = m_ref[...]
        new = jnp.maximum(old, jnp.max(s, axis=1, keepdims=True))
        scale = jnp.exp(old - new)
        w = jnp.exp(s - new)
        l_ref[...] = l_ref[...] * scale + jnp.sum(w, axis=1, keepdims=True)
        m_ref[...] = new
        w = w.astype(BF16)
        one = jnp.where(hit, 1.0, 0.0).astype(BF16)
        for t in range(0, D, tile):
            cols = pl.ds(t, tile)
            acc[:, cols] = acc[:, cols] * scale + dot_nn(w, block[:, cols])
            hit_acc[:, cols] += dot_nn(one, block[:, cols])

    slots = 2 * (half_ring - 1)

    def p_slot(i):
        d, chunk = 1 + i // 2, i % 2
        for way in range(2):
            src = origin(way, d)
            p_copy(way, src, d, chunk).wait_recv()

            @pl.when(d + 1 + (chunk + way) % 2 <= half_ring)
            def _():
                p_copy(way, src, d + 1, chunk).start()

    def use_p(j):
        use_passages(origin(j % 2, 1 + j // 2))

    use_passages(r)
    p_slot(0)
    p_slot(1)

    def p_step(i, carry):
        p_slot(i)
        use_p(i - 2)
        return carry

    lax.fori_loop(2, slots, p_step, 0)
    for chunk in range(2):
        for way in range(2):
            q_copy(way, r, 1, chunk).start()
    use_p(slots - 2)
    use_p(slots - 1)
    last = origin(0, half_ring)
    for way in range(2):
        p_copy(way, last, half_ring, way).wait_recv()
    use_passages(last)

    def q_slot(i):
        d, chunk = 1 + i // 2, i % 2
        for way in range(2):
            src = origin(way, d)
            q_copy(way, src, d, chunk).wait_recv()

            @pl.when(d + 1 + (chunk + way) % 2 <= half_ring)
            def _():
                q_copy(way, src, d + 1, chunk).start()

            f_copy(way, src, d, chunk, core).start()

    early = min(3, slots)

    def q_early(i):
        if i < early:
            q_slot(i)

    lane = lax.broadcasted_iota(jnp.int32, (Rq, 128), 1)
    cols = jnp.where(lane == 0, m_ref[...], jnp.where(lane == 1, l_ref[...], c_ref[...]))
    stats[...] = cols.T[0:8, :]

    def st_copy(k, src):
        return remote(stats, stats_in.at[src], st_send.at[k], st_recv.at[k],
                      to_grp((g + k) % G))

    for k in range(1, G):
        st_copy(k, g).start()
    q_early(0)
    for k in range(1, G):
        st_copy(k, (g - k + G) % G).wait_recv()
    stats_in[g] = stats[...]
    parts = [stats_in[k] for k in range(G)]
    top = functools.reduce(jnp.maximum, [v[0:1] for v in parts])
    total = functools.reduce(jnp.add, [v[1:2] * jnp.exp(v[0:1] - top) for v in parts])
    lse = top + jnp.log(total)
    loss_ref[...] = lse - functools.reduce(jnp.add, [v[2:3] for v in parts])
    lse_buf[...] = jnp.broadcast_to(lse, (8, Rq))

    def lse_copy(k, src):
        return remote(lse_buf, lse_all.at[src], lse_send.at[k], lse_recv.at[k],
                      to_row((r + k) % R))

    for k in range(1, R):
        lse_copy(k, r).start()
    lse_all[r] = lse_buf[...]

    lse_col = jnp.broadcast_to(lse, (128, Rq)).T[:, 0:1]
    hr = Rq // 2
    final = jnp.exp(m_ref[...] - lse_col)
    acc[...] = acc[...] * final - hit_acc[...]
    mine = pl.ds(pl.multiple_of(core * hr, hr), hr)
    other = pl.ds(pl.multiple_of((1 - core) * hr, hr), hr)
    core_copy = remote(acc.at[other], got_core, x_send.at[0], x_recv.at[0], to_grp(partner))
    core_copy.start()
    q_early(1)
    core_copy.wait_recv()
    half_sum[...] = acc[mine] + got_core[...]

    def y_copy(k):
        return remote(half_sum, got_y.at[k - 1], y_send.at[k], y_recv.at[k],
                      to_grp((g + 2 * k) % G))

    for k in range(1, G // 2):
        y_copy(k).start()

    q_early(2)

    gp_ref[...] = jnp.zeros((Pd, D), F32)
    base = (r * G + g) * Pd

    def use_queries(u):
        block = q_all.at[u]
        s = dot_nt(p_all[r], block[...])
        w = jnp.exp(s - lse_all[u][0:1]).astype(BF16)
        row = base + lax.broadcasted_iota(jnp.int32, (Pd, Rq), 0)
        one = jnp.where(row == pos_all[u][0:1], 1.0, 0.0).astype(BF16)
        for t in range(0, D, tile):
            c = pl.ds(t, tile)
            gp_ref[:, c] += dot_nn(w, block[:, c]) - dot_nn(one, block[:, c])

    def use_q(j):
        d, way = 1 + j // 2, j % 2
        src = origin(way, d)
        for chunk in range(2):
            f_copy(way, src, d, chunk, 1 - core).wait_recv()
        use_queries(src)

    for k in range(1, R):
        pos_copy(k, (r - k + R) % R).wait_recv()
        lse_copy(k, (r - k + R) % R).wait_recv()
    use_queries(r)

    def q_step(i, carry):
        q_slot(i)
        use_q(i - early)
        return carry

    lax.fori_loop(early, slots, q_step, 0)
    use_q(slots - early)
    for way in range(2):
        q_copy(way, last, half_ring, way).wait_recv()
        f_copy(way, last, half_ring, way, core).start()
    lax.fori_loop(slots - early + 1, slots - 1, lambda j, c: (use_q(j), c)[1], 0)

    for k in range(1, G // 2):
        y_copy(k).wait_recv()
    whole = half_sum[...]
    for k in range(1, G // 2):
        whole = whole + got_y[k - 1]
    done_half[...] = whole
    back_copy = remote(done_half, got_half, x_send.at[1], x_recv.at[1], to_grp(partner))
    back_copy.start()
    gq_ref[mine] = whole

    if early > 1:
        use_q(slots - 1)
    for way in range(2):
        f_copy(way, last, half_ring, way, 1 - core).wait_recv()
    use_queries(last)
    back_copy.wait_recv()
    gq_ref[other] = got_half[...]

    def drain(d, carry):
        for chunk in range(2):
            for way in range(2):
                src = origin(way, d)

                def settle():
                    p_copy(way, src, d, chunk).wait_send()
                    q_copy(way, src, d, chunk).wait_send()
                    f_copy(way, src, d, chunk, core).wait_send()

                if chunk == way:
                    settle()
                else:
                    pl.when(d < half_ring)(settle)
        return carry

    lax.fori_loop(1, half_ring + 1, drain, 0)
    for k in range(1, R):
        pos_copy(k, r).wait_send()
        lse_copy(k, r).wait_send()
    for k in range(1, G):
        st_copy(k, g).wait_send()
    for k in range(1, G // 2):
        y_copy(k).wait_send()
    core_copy.wait_send()
    back_copy.wait_send()


def local(R, G, queries, passages, positive):
    Rq, D = queries.shape
    Pd = passages.shape[0]
    ring = (2, R // 2 + 1, 2)
    sem = pltpu.SemaphoreType.DMA
    vmem = pltpu.VMEM
    losses, gq, gp = pl.pallas_call(
        functools.partial(kernel, R, G),
        out_shape=(
            jax.ShapeDtypeStruct((1, Rq), F32),
            jax.ShapeDtypeStruct((Rq, D), F32),
            jax.ShapeDtypeStruct((Pd, D), F32),
        ),
        in_specs=[
            pl.BlockSpec(memory_space=pl.ANY),
            pl.BlockSpec(memory_space=pl.ANY),
            pl.BlockSpec(memory_space=vmem),
        ],
        out_specs=[pl.BlockSpec(memory_space=vmem)] * 3,
        scratch_shapes=[
            vmem((R, Pd, D), BF16),
            vmem((R, Rq, D), BF16),
            vmem((R, 8, Rq), jnp.int32),
            vmem((R, 8, Rq), F32),
            vmem((8, Rq), F32),
            vmem((G, 8, Rq), F32),
            vmem((8, Rq), F32),
            vmem((Rq, D), F32),
            vmem((Rq, D), F32),
            vmem((Rq, 1), F32),
            vmem((Rq, 1), F32),
            vmem((Rq, 1), F32),
            vmem((Rq, 1), jnp.int32),
            vmem((8, Rq), jnp.int32),
            vmem((Rq // 2, D), F32),
            vmem((Rq // 2, D), F32),
            vmem((G // 2 - 1, Rq // 2, D), F32),
            vmem((Rq // 2, D), F32),
            vmem((Rq // 2, D), F32),
            sem((2,)),
            sem(ring), sem(ring), sem(ring), sem(ring), sem(ring), sem(ring),
            sem((R,)), sem((R,)), sem((R,)), sem((R,)), sem((G,)), sem((G,)),
            sem((2,)), sem((2,)), sem((G // 2,)), sem((G // 2,)),
        ],
        compiler_params=pltpu.CompilerParams(
            collective_id=0, has_side_effects=True, vmem_limit_bytes=min(R * (Pd + Rq) * D * 2 + 16 * Rq * D * 4, 60 * 1024 * 1024)
        ),
        name="infonce",
    )(queries, passages, positive[None, :])
    return losses[0], gq, gp


def solution(mesh):
    R, G = mesh.shape["rows"], mesh.shape["grp"]
    return jax.shard_map(
        functools.partial(local, R, G),
        mesh=mesh,
        in_specs=(P("rows", None), P(("rows", "grp"), None), P("rows")),
        out_specs=(P("rows"), P("rows", None), P(("rows", "grp"), None)),
        check_vma=False,
    )
```

```python
import functools

import jax
import jax.numpy as jnp
from jax import lax
from jax.experimental import pallas as pl
from jax.experimental.pallas import tpu as pltpu
from jax.sharding import PartitionSpec as P

lowest = -1e30
MESH = pl.DeviceIdType.MESH
F32 = jnp.float32
BF16 = jnp.bfloat16


def dot_nt(a, b):
    return lax.dot_general(a, b, (((1,), (1,)), ((), ())), preferred_element_type=F32)


def dot_nn(a, b):
    return jnp.dot(a, b, preferred_element_type=F32)


def kernel(
    R, G, q_hbm, p_hbm, pos_ref,
    loss_ref, gq_ref, gp_ref,
    p_all, q_all, pos_all, lse_all, stats, stats_in, lse_buf,
    acc, hit_acc, m_ref, l_ref, c_ref, final_ref, pos_col_ref, pos_row_ref,
    got_core, half_sum, got_y, done_half, got_half,
    local_sem, p_send, p_recv, q_send, q_recv, f_send, f_recv,
    pos_send, pos_recv, lse_send, lse_recv, st_send, st_recv,
    x_send, x_recv, y_send, y_recv,
):
    r = lax.axis_index("rows")
    g = lax.axis_index("grp")
    half_ring = R // 2
    _, Pd, D = p_all.shape
    Rq = q_all.shape[1]
    tile = min(256, D)
    z, x = r // 2, r % 2
    place = z + x * (R - 1 - 2 * z)

    def row_of(where):
        far = where // half_ring
        return 2 * (where + far * (R - 1 - 2 * where)) + far

    def origin(way, d):
        return row_of((place + (2 * way - 1) * d + R) % R)

    right, left = row_of((place + 1) % R), row_of((place + R - 1) % R)
    target = (right, left)
    core = g % 2
    partner = g + 1 - 2 * core

    def to_row(row):
        return (row, g)

    def to_grp(col):
        return (r, col)

    def remote(src, dst, send, recv, device):
        return pltpu.make_async_remote_copy(
            src_ref=src, dst_ref=dst, send_sem=send, recv_sem=recv,
            device_id=device, device_id_type=MESH,
        )

    load_p = pltpu.make_async_copy(p_hbm, p_all.at[r], local_sem.at[0])
    load_q = pltpu.make_async_copy(q_hbm, q_all.at[r], local_sem.at[1])
    load_p.start()
    load_q.start()

    barrier = pltpu.get_barrier_semaphore()
    for k in range(1, R):
        pl.semaphore_signal(barrier, inc=1, device_id=to_row((r + k) % R), device_id_type=MESH)
    for k in range(1, G):
        pl.semaphore_signal(barrier, inc=1, device_id=to_grp((g + k) % G), device_id_type=MESH)
    pl.semaphore_wait(barrier, R - 1 + G - 1)

    pc = Pd // 2

    def p_copy(way, src, d, chunk):
        piece = p_all.at[src, pl.ds(chunk * pc, pc)]
        return remote(piece, piece, p_send.at[way, d, chunk], p_recv.at[way, d, chunk],
                      to_row(target[way]))

    qc = Rq // 4

    def q_copy(way, src, d, chunk):
        piece = q_all.at[src, pl.ds(pl.multiple_of(core * (2 * qc) + chunk * qc, qc), qc)]
        return remote(piece, piece, q_send.at[way, d, chunk], q_recv.at[way, d, chunk],
                      to_row(target[way]))

    def f_copy(way, src, d, chunk, whose):
        piece = q_all.at[src, pl.ds(pl.multiple_of(whose * (2 * qc) + chunk * qc, qc), qc)]
        return remote(piece, piece, f_send.at[way, d, chunk], f_recv.at[way, d, chunk],
                      to_grp(partner))

    load_p.wait()
    for chunk in range(2):
        for way in range(2):
            p_copy(way, r, 1, chunk).start()
    load_q.wait()

    def pos_copy(k, src):
        return remote(pos_row_ref, pos_all.at[src], pos_send.at[k], pos_recv.at[k],
                      to_row((r + k) % R))

    pos_row_ref[...] = jnp.broadcast_to(pos_ref[...], (8, Rq))
    pos_col_ref[...] = jnp.broadcast_to(pos_ref[...], (128, Rq)).T[:, 0:1]
    for k in range(1, R):
        pos_copy(k, r).start()
    pos_all[r] = pos_row_ref[...]

    m_ref[...] = jnp.full((Rq, 1), lowest, F32)
    l_ref[...] = jnp.zeros((Rq, 1), F32)
    c_ref[...] = jnp.zeros((Rq, 1), F32)
    acc[...] = jnp.zeros((Rq, D), F32)
    hit_acc[...] = jnp.zeros((Rq, D), F32)

    def use_passages(u, between=None):
        block = p_all.at[u]
        s = dot_nt(q_all[r], block[...])
        column = (u * G + g) * Pd + lax.broadcasted_iota(jnp.int32, (Rq, Pd), 1)
        hit = pos_col_ref[...] == column
        c_ref[...] += jnp.sum(jnp.where(hit, s, 0.0), axis=1, keepdims=True)
        old = m_ref[...]
        new = jnp.maximum(old, jnp.max(s, axis=1, keepdims=True))
        scale = jnp.exp(old - new)
        w = jnp.exp(s - new)
        l_ref[...] = l_ref[...] * scale + jnp.sum(w, axis=1, keepdims=True)
        m_ref[...] = new
        if between is not None:
            between()
        w = w.astype(BF16)
        one = jnp.where(hit, 1.0, 0.0).astype(BF16)
        for t in range(0, D, tile):
            cols = pl.ds(t, tile)
            acc[:, cols] = acc[:, cols] * scale + dot_nn(w, block[:, cols])
            hit_acc[:, cols] += dot_nn(one, block[:, cols])

    slots = 2 * (half_ring - 1)

    def p_slot(i):
        d, chunk = 1 + i // 2, i % 2
        for way in range(2):
            src = origin(way, d)
            p_copy(way, src, d, chunk).wait_recv()

            @pl.when(d + 1 + (chunk + way) % 2 <= half_ring)
            def _():
                p_copy(way, src, d + 1, chunk).start()

    def use_p(j):
        use_passages(origin(j % 2, 1 + j // 2))

    use_passages(r)
    p_slot(0)
    p_slot(1)

    def p_step(i, carry):
        p_slot(i)
        use_p(i - 2)
        return carry

    lax.fori_loop(2, slots, p_step, 0)
    for chunk in range(2):
        for way in range(2):
            q_copy(way, r, 1, chunk).start()
    use_p(slots - 2)
    use_p(slots - 1)
    last = origin(0, half_ring)
    for way in range(2):
        p_copy(way, last, half_ring, way).wait_recv()

    def st_copy(k, src):
        return remote(stats, stats_in.at[src], st_send.at[k], st_recv.at[k],
                      to_grp((g + k) % G))

    def send_stats():
        lane = lax.broadcasted_iota(jnp.int32, (Rq, 128), 1)
        cols = jnp.where(lane == 0, m_ref[...], jnp.where(lane == 1, l_ref[...], c_ref[...]))
        stats[...] = cols.T[0:8, :]
        for k in range(1, G):
            st_copy(k, g).start()

    use_passages(last, send_stats)

    def q_slot(i):
        d, chunk = 1 + i // 2, i % 2
        for way in range(2):
            src = origin(way, d)
            q_copy(way, src, d, chunk).wait_recv()

            @pl.when(d + 1 + (chunk + way) % 2 <= half_ring)
            def _():
                q_copy(way, src, d + 1, chunk).start()

            f_copy(way, src, d, chunk, core).start()

    early = min(3, slots)

    def q_early(i):
        if i < early:
            q_slot(i)

    for k in range(1, G):
        st_copy(k, (g - k + G) % G).wait_recv()
    stats_in[g] = stats[...]
    parts = [stats_in[k] for k in range(G)]
    top = functools.reduce(jnp.maximum, [v[0:1] for v in parts])
    total = functools.reduce(jnp.add, [v[1:2] * jnp.exp(v[0:1] - top) for v in parts])
    lse = top + jnp.log(total)
    loss_ref[...] = lse - functools.reduce(jnp.add, [v[2:3] for v in parts])
    lse_buf[...] = jnp.broadcast_to(lse, (8, Rq))

    def lse_copy(k, src):
        return remote(lse_buf, lse_all.at[src], lse_send.at[k], lse_recv.at[k],
                      to_row((r + k) % R))

    for k in range(1, R):
        lse_copy(k, r).start()
    lse_all[r] = lse_buf[...]

    lse_col = jnp.broadcast_to(lse, (128, Rq)).T[:, 0:1]
    hr = Rq // 2
    final_ref[...] = jnp.exp(m_ref[...] - lse_col)
    pieces = got_core.shape[0]
    pr = hr // pieces

    def piece_of(whose, n):
        return pl.ds(pl.multiple_of(whose * hr + n * pr, pr), pr)

    def core_copy(n):
        return remote(acc.at[piece_of(1 - core, n)], got_core.at[n],
                      x_send.at[0, n], x_recv.at[0, n], to_grp(partner))

    def y_copy(k, n):
        return remote(half_sum.at[n], got_y.at[k - 1, n], y_send.at[k, n], y_recv.at[k, n],
                      to_grp((g + 2 * k) % G))

    def back_copy(n):
        return remote(done_half.at[n], got_half.at[n], x_send.at[1, n], x_recv.at[1, n],
                      to_grp(partner))

    for n in range(pieces):
        at = piece_of(1 - core, n)
        acc[at] = acc[at] * final_ref[at] - hit_acc[at]
        core_copy(n).start()
    for n in range(pieces):
        at = piece_of(core, n)
        acc[at] = acc[at] * final_ref[at] - hit_acc[at]
    q_early(0)
    for n in range(pieces):
        core_copy(n).wait_recv()
        half_sum[n] = acc[piece_of(core, n)] + got_core[n]
        for k in range(1, G // 2):
            y_copy(k, n).start()
    q_early(1)
    q_early(2)

    def finish_piece(n):
        whole = half_sum[n]
        for k in range(1, G // 2):
            y_copy(k, n).wait_recv()
            whole = whole + got_y[k - 1, n]
        done_half[n] = whole
        back_copy(n).start()
        gq_ref[piece_of(core, n)] = whole

    gp_ref[...] = jnp.zeros((Pd, D), F32)
    base = (r * G + g) * Pd

    def use_queries(u):
        block = q_all.at[u]
        s = dot_nt(p_all[r], block[...])
        w = jnp.exp(s - lse_all[u][0:1]).astype(BF16)
        row = base + lax.broadcasted_iota(jnp.int32, (Pd, Rq), 0)
        one = jnp.where(row == pos_all[u][0:1], 1.0, 0.0).astype(BF16)
        for t in range(0, D, tile):
            c = pl.ds(t, tile)
            gp_ref[:, c] += dot_nn(w, block[:, c]) - dot_nn(one, block[:, c])

    def use_q(j):
        d, way = 1 + j // 2, j % 2
        src = origin(way, d)
        for chunk in range(2):
            f_copy(way, src, d, chunk, 1 - core).wait_recv()
        use_queries(src)

    for k in range(1, R):
        pos_copy(k, (r - k + R) % R).wait_recv()
        lse_copy(k, (r - k + R) % R).wait_recv()
    use_queries(r)

    def q_step(i, carry):
        q_slot(i)
        use_q(i - early)
        return carry

    unrolled = min(early + pieces - 1, slots)
    for i in range(early, unrolled):
        q_step(i, 0)
        finish_piece(i - early)
    lax.fori_loop(unrolled, slots, q_step, 0)
    use_q(slots - early)
    for way in range(2):
        q_copy(way, last, half_ring, way).wait_recv()
        f_copy(way, last, half_ring, way, core).start()
    for n in range(unrolled - early, pieces):
        finish_piece(n)
    lax.fori_loop(slots - early + 1, slots, lambda j, c: (use_q(j), c)[1], 0)
    for way in range(2):
        f_copy(way, last, half_ring, way, 1 - core).wait_recv()
    use_queries(last)
    for n in range(pieces):
        back_copy(n).wait_recv()
        gq_ref[piece_of(1 - core, n)] = got_half[n]

    def drain(d, carry):
        for chunk in range(2):
            for way in range(2):
                src = origin(way, d)

                def settle():
                    p_copy(way, src, d, chunk).wait_send()
                    q_copy(way, src, d, chunk).wait_send()
                    f_copy(way, src, d, chunk, core).wait_send()

                if chunk == way:
                    settle()
                else:
                    pl.when(d < half_ring)(settle)
        return carry

    lax.fori_loop(1, half_ring + 1, drain, 0)
    for k in range(1, R):
        pos_copy(k, r).wait_send()
        lse_copy(k, r).wait_send()
    for k in range(1, G):
        st_copy(k, g).wait_send()
    for n in range(pieces):
        for k in range(1, G // 2):
            y_copy(k, n).wait_send()
        core_copy(n).wait_send()
        back_copy(n).wait_send()


def local(R, G, queries, passages, positive):
    Rq, D = queries.shape
    Pd = passages.shape[0]
    ring = (2, R // 2 + 1, 2)
    pieces = 4
    pr = Rq // 2 // pieces
    sem = pltpu.SemaphoreType.DMA
    vmem = pltpu.VMEM
    losses, gq, gp = pl.pallas_call(
        functools.partial(kernel, R, G),
        out_shape=(
            jax.ShapeDtypeStruct((1, Rq), F32),
            jax.ShapeDtypeStruct((Rq, D), F32),
            jax.ShapeDtypeStruct((Pd, D), F32),
        ),
        in_specs=[
            pl.BlockSpec(memory_space=pltpu.HBM),
            pl.BlockSpec(memory_space=pltpu.HBM),
            pl.BlockSpec(memory_space=vmem),
        ],
        out_specs=[pl.BlockSpec(memory_space=vmem)] * 3,
        scratch_shapes=[
            vmem((R, Pd, D), BF16),
            vmem((R, Rq, D), BF16),
            vmem((R, 8, Rq), jnp.int32),
            vmem((R, 8, Rq), F32),
            vmem((8, Rq), F32),
            vmem((G, 8, Rq), F32),
            vmem((8, Rq), F32),
            vmem((Rq, D), F32),
            vmem((Rq, D), F32),
            vmem((Rq, 1), F32),
            vmem((Rq, 1), F32),
            vmem((Rq, 1), F32),
            vmem((Rq, 1), F32),
            vmem((Rq, 1), jnp.int32),
            vmem((8, Rq), jnp.int32),
            vmem((pieces, pr, D), F32),
            vmem((pieces, pr, D), F32),
            vmem((G // 2 - 1, pieces, pr, D), F32),
            vmem((pieces, pr, D), F32),
            vmem((pieces, pr, D), F32),
            sem((2,)),
            sem(ring), sem(ring), sem(ring), sem(ring), sem(ring), sem(ring),
            sem((R,)), sem((R,)), sem((R,)), sem((R,)), sem((G,)), sem((G,)),
            sem((2, pieces)), sem((2, pieces)), sem((G // 2, pieces)), sem((G // 2, pieces)),
        ],
        compiler_params=pltpu.CompilerParams(
            collective_id=0, has_side_effects=True, vmem_limit_bytes=min(R * (Pd + Rq) * D * 2 + 16 * Rq * D * 4, 60 * 1024 * 1024)
        ),
        name="infonce",
    )(queries, passages, positive[None, :])
    return losses[0], gq, gp


def solution(mesh):
    R, G = mesh.shape["rows"], mesh.shape["grp"]
    return jax.shard_map(
        functools.partial(local, R, G),
        mesh=mesh,
        in_specs=(P("rows", None), P(("rows", "grp"), None), P("rows")),
        out_specs=(P("rows"), P("rows", None), P(("rows", "grp"), None)),
        check_vma=False,
    )
```
